32 devices in a mesh: py: 2 (over x), px: 4 (over z), pz: 4 (over y, core).
Axes of the slice: x: 2, y: 2, z: 4, core: 2. Of those that a mesh axis runs over, the one named last changes fastest.
Arguments:
- field_now: float32 [16, 64, 256, 128], P('py', 'px', 'pz'), may hold values from 0.2 to 1.8
- earlier: float32 [16, 64, 256, 128], P('py', 'px', 'pz'), may hold values from 0.2 to 1.8
- speed_square: float32 [16, 64, 256, 128], P('py', 'px', 'pz'), may hold values from 0.05 to 0.3
Outputs:
- column_sum: float32 [16, 64, 256, 128], P('py', 'px', 'pz')
- field_now_end: float32 [16, 64, 256, 128], P('py', 'px', 'pz')
The draws below stay inside these ranges and needn't reach their ends.
All inputs are finite; a program needn't handle non-finite values.
Results may differ from the reference program's by a relative error of at most 0.00002.
Values sent between devices are 32-bit elements; how exact they have to be, the bound alone decides.
No kernel may reach another device: no remote copies, remote signals or barrier semaphores. Data moves between devices by JAX's collectives and lax.ppermute only.
A program may use at most 128 MiB of HBM per device.

```python
import jax
import jax.numpy as jnp
from jax import lax

GRID_J = 16
GRID_I = 64
GRID_K = 256
LEVELS = 128
STEPS = 4


def shard_levels(key, extent, split, low, top_value):
    level = 1.0
    for position, shards_of in split:
        heights = jax.random.uniform(jax.random.fold_in(jax.random.fold_in(key, 6), position), (shards_of,), jnp.float32, low / len(split), top_value / len(split))
        level = level * jnp.repeat(jnp.exp(heights), extent[position] // shards_of).reshape((-1,) + (1,) * (len(extent) - 1 - position))
    return level


def setup_inputs(seed: int = 0) -> dict:
    seeds = jax.random.split(jax.random.key(seed), 4)
    field_now = jnp.clip(0.2 + 1.5999999 * jax.random.uniform(seeds[0], (GRID_J, GRID_I, GRID_K, LEVELS), jnp.float32) ** shard_levels(seeds[0], (GRID_J, GRID_I, GRID_K, LEVELS), ((0, 2), (1, 4), (2, 4)), -0.2, 0.2), 0.2, 1.8)
    earlier = jnp.clip(0.2 + 1.5999999 * jax.random.uniform(seeds[1], (GRID_J, GRID_I, GRID_K, LEVELS), jnp.float32) ** shard_levels(seeds[1], (GRID_J, GRID_I, GRID_K, LEVELS), ((0, 2), (1, 4), (2, 4)), -0.2, 0.2), 0.2, 1.8)
    speed_square = jnp.clip(0.05 + 0.25 * jax.random.uniform(seeds[2], (GRID_J, GRID_I, GRID_K, LEVELS), jnp.float32) ** shard_levels(seeds[2], (GRID_J, GRID_I, GRID_K, LEVELS), ((0, 2), (1, 4), (2, 4)), -0.2, 0.2), 0.05, 0.3)
    return dict(field_now=field_now, earlier=earlier, speed_square=speed_square)


def without_rim(values, dims):
    for dim in dims:
        values = lax.slice_in_dim(values, 1, values.shape[dim] - 1, axis=dim)
    return values


def shifted_cells(values, dim, start, dims):
    others = [other for other in dims if other != dim]
    values = without_rim(values, others)
    return lax.slice_in_dim(values, start, start + values.shape[dim] - 2, axis=dim)


def march_step(padded, before, speed_square):
    middle = without_rim(padded, (0, 1, 2))
    lower = [shifted_cells(padded, dim, 0, (0, 1, 2)) for dim in (0, 1, 2)]
    upper = [shifted_cells(padded, dim, 2, (0, 1, 2)) for dim in (0, 1, 2)]
    spread = lower[0] + upper[0] + lower[1] + upper[1] + lower[2] + upper[2] - 6.0 * middle
    return 2.0 * middle - before + speed_square * spread


def reference(field_now, earlier, speed_square):
    for step in range(STEPS):
        later = march_step(jnp.pad(field_now, ((1, 1), (1, 1), (1, 1), (0, 0)), mode="wrap"), earlier, speed_square)
        earlier, field_now = field_now, later
    column_sum = jnp.cumsum(field_now, axis=0) / GRID_J
    return column_sum, field_now
```

```python
import functools

import jax
import jax.numpy as jnp
from jax import lax
from jax.experimental import pallas as pl
from jax.experimental.pallas import tpu as pltpu
from jax.sharding import PartitionSpec as P

STEPS = 4
VMEM_LIMIT = 40 * 1024 * 1024
F32 = jnp.float32


def ring(axis, step):
    peers = lax.axis_size(axis)
    return [(i, (i + step) % peers) for i in range(peers)]


def shift_up(value, axis):
    return lax.ppermute(value, axis, ring(axis, 1))


def shift_down(value, axis):
    return lax.ppermute(value, axis, ring(axis, -1))


def update_row(at, below, above, before, speed, i_low, i_high, k_low, k_high, put):
    size, depth = i_low.shape[-2:], k_low.shape[0]
    place = lax.broadcasted_iota(jnp.int32, size, 0)
    first, last = place == 0, place == size[0] - 1
    for i in range(depth):
        middle = at(i)
        low = i_low[...] if i == 0 else at(i - 1)
        high = i_high[...] if i == depth - 1 else at(i + 1)
        back = jnp.where(first, k_low[i : i + 1, :], pltpu.roll(middle, 1, 0))
        ahead = jnp.where(last, k_high[i : i + 1, :], pltpu.roll(middle, size[0] - 1, 0))
        spread = below(i) + above(i) + low + high + back + ahead - 6.0 * middle
        put(i, 2.0 * middle - before(i) + speed(i) * spread)


def step_kernel(kind, names_in, names_out, *refs):
    r = dict(zip(names_in + names_out, refs))
    if kind == "middle":
        row = pl.program_id(0) + 1
        at = lambda i: r["u"][row, i]
        below = lambda i: r["u"][row - 1, i]
        above = lambda i: r["u"][row + 1, i]
    else:
        at = lambda i: r["u"][0, i]
        inner = lambda i: r["u_next"][0, i]
        outer = lambda i: r["halo"][0, i]
        below, above = (outer, inner) if kind == "first" else (inner, outer)
    depth = r["k_low"].shape[1]
    width = r["i_low"].shape[2]

    if kind == "middle" and "sum_out" in r:

        @pl.when(pl.program_id(0) == 0)
        def _():
            r["sum_out"][...] = r["sum_in"][...]

    def put(i, new):
        r["new"][0, i] = new
        if "row" in r:
            r["row"][0, i] = new
        if "sum_out" in r:
            source = r["sum_out"] if kind == "middle" else r["sum_in"]
            r["sum_out"][0, i] = source[0, i] + new
        if "send_i_low" in r:
            if i == 0:
                r["send_i_low"][0, 0] = new
            if i == depth - 1:
                r["send_i_high"][0, 0] = new
            r["send_k_low"][0, i : i + 1, :] = new[:1]
            r["send_k_high"][0, i : i + 1, :] = new[width - 1 :]

    update_row(
        at, below, above, lambda i: r["e"][0, i], lambda i: r["s"][0, i],
        r["i_low"].at[0, 0], r["i_high"].at[0, 0], r["k_low"].at[0], r["k_high"].at[0], put,
    )


FACES = ("send_i_low", "send_i_high", "send_k_low", "send_k_high")


def update(kind, u, e, s, halos, halo, state, in_place, send, row_out, sum_in):
    n, depth, width, levels = u.shape
    start = {"first": 0, "middle": 1, "last": n - 1}[kind]
    count = n - 2 if kind == "middle" else 1
    line = pl.BlockSpec((1, depth, width, levels), lambda j: (j + start, 0, 0, 0))
    alone = pl.BlockSpec((1, depth, width, levels), lambda j: (0, 0, 0, 0))
    face_i = pl.BlockSpec((1, 1, width, levels), lambda j: (j + start, 0, 0, 0))
    face_k = pl.BlockSpec((1, depth, levels), lambda j: (j + start, 0, 0))
    anywhere = pl.BlockSpec(memory_space=pl.ANY)
    ins = []
    if kind == "middle":
        ins.append(("u", u, pl.BlockSpec(u.shape, lambda j: (0, 0, 0, 0))))
    else:
        inner = start + 1 if kind == "first" else start - 1
        ins.append(("u", u, line))
        ins.append(("u_next", u, pl.BlockSpec((1, depth, width, levels), lambda j: (inner, 0, 0, 0))))
        ins.append(("halo", halo, alone))
    source = state["new"] if (in_place and state) else e
    ins += [("e", source, line), ("s", s, line)]
    ins += [("i_low", halos[0], face_i), ("i_high", halos[1], face_i)]
    ins += [("k_low", halos[2], face_k), ("k_high", halos[3], face_k)]
    if sum_in is not None:
        ins.append(("sum_in", sum_in, alone))
    outs = [("new", jax.ShapeDtypeStruct(u.shape, F32), line)]
    if send:
        face = jax.ShapeDtypeStruct((n, 1, width, levels), F32)
        strip = jax.ShapeDtypeStruct((n, depth, levels), F32)
        outs += list(zip(FACES, (face, face, strip, strip), (face_i, face_i, face_k, face_k)))
    if row_out:
        outs.append(("row", jax.ShapeDtypeStruct((1, depth, width, levels), F32), alone))
    if sum_in is not None:
        outs.append(("sum_out", jax.ShapeDtypeStruct((1, depth, width, levels), F32), alone))
    aliases = {}
    where_out = {name: index for index, (name, _, _) in enumerate(outs)}
    if in_place:
        aliases[[name for name, _, _ in ins].index("e")] = 0
    if state:
        for name, value in state.items():
            if name not in where_out or (name == "new" and in_place):
                continue
            aliases[len(ins)] = where_out[name]
            ins.append(("old_" + name, value, anywhere))
    names_in, names_out = tuple(x[0] for x in ins), tuple(x[0] for x in outs)
    cells = count * depth * width * levels
    results = pl.pallas_call(
        functools.partial(step_kernel, kind, names_in, names_out),
        grid=(count,),
        in_specs=[x[2] for x in ins],
        out_specs=[x[2] for x in outs],
        out_shape=[x[1] for x in outs],
        input_output_aliases=aliases,
        compiler_params=pltpu.CompilerParams(
            vmem_limit_bytes=VMEM_LIMIT, dimension_semantics=("arbitrary",)
        ),
        cost_estimate=pl.CostEstimate(flops=40 * cells, bytes_accessed=20 * cells, transcendentals=0),
        name="rows_" + kind,
    )(*[x[1] for x in ins])
    return dict(zip(names_out, results))


def sums_kernel(scale, u_ref, below_ref, out_ref):
    n, depth = u_ref.shape[:2]
    for i in range(depth):
        total = below_ref[0, i]
        for j in range(n):
            total = total + u_ref[j, i]
            out_ref[j, i] = total * scale


def column_sums(u, below, scale):
    n, depth, width, levels = u.shape
    part = 2 if depth % 2 == 0 else 1
    block = pl.BlockSpec((n, part, width, levels), lambda i: (0, i, 0, 0))
    return pl.pallas_call(
        functools.partial(sums_kernel, scale),
        grid=(depth // part,),
        in_specs=[block, pl.BlockSpec((1, part, width, levels), lambda i: (0, i, 0, 0))],
        out_specs=block,
        out_shape=jax.ShapeDtypeStruct(u.shape, F32),
        compiler_params=pltpu.CompilerParams(
            vmem_limit_bytes=VMEM_LIMIT, dimension_semantics=("arbitrary",)
        ),
        cost_estimate=pl.CostEstimate(flops=40 * u.size, bytes_accessed=8 * u.size, transcendentals=0),
        name="column_sums",
    )(u, below)


def exchange(faces):
    i_low, i_high, k_low, k_high = faces
    return (
        shift_up(i_high, "px"), shift_down(i_low, "px"),
        shift_up(k_high, "pz"), shift_down(k_low, "pz"),
    )


def local(field_now, earlier, speed_square):
    n, depth, width, _ = field_now.shape
    u, e, s = field_now, earlier, speed_square
    before = shift_up(u[n - 1 :], "py")
    after = shift_down(u[:1], "py")
    halos = exchange((u[:, :1], u[:, depth - 1 :], u[:, :, 0], u[:, :, width - 1]))
    for step in range(STEPS):
        ending = step == STEPS - 1
        order = ("first", "middle", "last") if step % 2 == 0 else ("last", "middle", "first")
        state, total, rows = None, None, {}
        for kind in order:
            result = update(
                kind, u, e, s, halos, {"first": before, "last": after}.get(kind), state,
                step >= 2, not ending, kind != "middle" and not (ending and kind == order[2]),
                total if ending else None,
            )
            if kind != "middle" and "row" in result:
                rows[kind] = result["row"]
            if ending:
                total = result.get("sum_out", result.get("row"))
            state = {name: result[name] for name in ("new",) + FACES if name in result}
        e, u = u, state["new"]
        if not ending:
            before = shift_up(rows["last"], "py")
            after = shift_down(rows["first"], "py")
            halos = exchange([state[name] for name in FACES])
    peers = lax.axis_size("py")
    below = lax.ppermute(total, "py", [(i, i + 1) for i in range(peers - 1)])
    reach = 1
    while reach < peers - 1:
        below = below + lax.ppermute(below, "py", [(i, i + reach) for i in range(peers - reach)])
        reach *= 2
    return column_sums(u, below, 1.0 / (n * peers)), u


def solution(mesh):
    placed = P("py", "px", "pz", None)
    return jax.shard_map(
        local, mesh=mesh, in_specs=(placed, placed, placed), out_specs=(placed, placed), check_vma=False
    )
```

```python
import functools

import jax
import jax.numpy as jnp
from jax import lax
from jax.experimental import pallas as pl
from jax.experimental.pallas import tpu as pltpu
from jax.sharding import PartitionSpec as P

STEPS = 4
VMEM_LIMIT = 16 * 1024 * 1024
STAGE_LIMIT = 44 * 1024 * 1024
F32 = jnp.float32


def ring(axis, step):
    peers = lax.axis_size(axis)
    return [(i, (i + step) % peers) for i in range(peers)]


def shift_up(value, axis):
    return lax.ppermute(value, axis, ring(axis, 1))


def shift_down(value, axis):
    return lax.ppermute(value, axis, ring(axis, -1))


def update_row(at, below, above, before, speed, i_low, i_high, k_low, k_high, put):
    size, depth = i_low.shape[-2:], k_low.shape[0]
    place = lax.broadcasted_iota(jnp.int32, size, 0)
    first, last = place == 0, place == size[0] - 1
    for i in range(depth):
        middle = at(i)
        low = i_low[...] if i == 0 else at(i - 1)
        high = i_high[...] if i == depth - 1 else at(i + 1)
        back = jnp.where(first, k_low[i : i + 1, :], pltpu.roll(middle, 1, 0))
        ahead = jnp.where(last, k_high[i : i + 1, :], pltpu.roll(middle, size[0] - 1, 0))
        spread = below(i) + above(i) + low + high + back + ahead - 6.0 * middle
        put(i, 2.0 * middle - before(i) + speed(i) * spread)


def step_kernel(kind, names_in, names_out, *refs):
    r = dict(zip(names_in + names_out, refs))
    if kind == "middle":
        row = pl.program_id(0) + 1
        at = lambda i: r["u"][row, i]
        below = lambda i: r["u"][row - 1, i]
        above = lambda i: r["u"][row + 1, i]
    else:
        at = lambda i: r["u"][0, i]
        inner = lambda i: r["u_next"][0, i]
        outer = lambda i: r["halo"][0, i]
        below, above = (outer, inner) if kind == "first" else (inner, outer)
    depth = r["k_low"].shape[1]
    width = r["i_low"].shape[2]

    if kind == "middle" and "sum_out" in r:

        @pl.when(pl.program_id(0) == 0)
        def _():
            r["sum_out"][...] = r["sum_in"][...]

    def put(i, new):
        r["new"][0, i] = new
        if "row" in r:
            r["row"][0, i] = new
        if "sum_out" in r:
            r["sum_out"][0, i] = r["sum_out"][0, i] + new
        if "sum_low" in r:
            half = r["sum_low"].shape[1]
            target = r["sum_low"].at[0, i] if i < half else r["sum_high"].at[0, i - half]
            target[...] = r["sum_in"][0, i] + new
        if "send_i_low" in r:
            if i == 0:
                r["send_i_low"][0, 0] = new
            if i == depth - 1:
                r["send_i_high"][0, 0] = new
            r["send_k_low"][0, i : i + 1, :] = new[:1]
            r["send_k_high"][0, i : i + 1, :] = new[width - 1 :]

    update_row(
        at, below, above, lambda i: r["e"][0, i], lambda i: r["s"][0, i],
        r["i_low"].at[0, 0], r["i_high"].at[0, 0], r["k_low"].at[0], r["k_high"].at[0], put,
    )


FACES = ("send_i_low", "send_i_high", "send_k_low", "send_k_high")


def update(kind, u, e, s, halos, halo, state, in_place, send, row_out, sum_in):
    n, depth, width, levels = u.shape
    start = {"first": 0, "middle": 1, "last": n - 1}[kind]
    count = n - 2 if kind == "middle" else 1
    line = pl.BlockSpec((1, depth, width, levels), lambda j: (j + start, 0, 0, 0))
    alone = pl.BlockSpec((1, depth, width, levels), lambda j: (0, 0, 0, 0))
    face_i = pl.BlockSpec((1, 1, width, levels), lambda j: (j + start, 0, 0, 0))
    face_k = pl.BlockSpec((1, depth, levels), lambda j: (j + start, 0, 0))
    anywhere = pl.BlockSpec(memory_space=pl.ANY)
    ins = []
    if kind == "middle":
        ins.append(("u", u, pl.BlockSpec(u.shape, lambda j: (0, 0, 0, 0))))
    else:
        inner = start + 1 if kind == "first" else start - 1
        ins.append(("u", u, line))
        ins.append(("u_next", u, pl.BlockSpec((1, depth, width, levels), lambda j: (inner, 0, 0, 0))))
        ins.append(("halo", halo, alone))
    source = state["new"] if (in_place and state) else e
    ins += [("e", source, line), ("s", s, line)]
    ins += [("i_low", halos[0], face_i), ("i_high", halos[1], face_i)]
    ins += [("k_low", halos[2], face_k), ("k_high", halos[3], face_k)]
    if sum_in is not None:
        ins.append(("sum_in", sum_in, alone))
    outs = [("new", jax.ShapeDtypeStruct(u.shape, F32), line)]
    if send:
        face = jax.ShapeDtypeStruct((n, 1, width, levels), F32)
        strip = jax.ShapeDtypeStruct((n, depth, levels), F32)
        outs += list(zip(FACES, (face, face, strip, strip), (face_i, face_i, face_k, face_k)))
    if row_out:
        outs.append(("row", jax.ShapeDtypeStruct((1, depth, width, levels), F32), alone))
    if sum_in is not None and kind == "middle":
        outs.append(("sum_out", jax.ShapeDtypeStruct((1, depth, width, levels), F32), alone))
    elif sum_in is not None:
        for name, size in (("sum_low", depth // 2), ("sum_high", depth - depth // 2)):
            part = (1, size, width, levels)
            outs.append((name, jax.ShapeDtypeStruct(part, F32), pl.BlockSpec(part, lambda j: (0, 0, 0, 0))))
    aliases = {}
    where_out = {name: index for index, (name, _, _) in enumerate(outs)}
    if in_place:
        aliases[[name for name, _, _ in ins].index("e")] = 0
    if state:
        for name, value in state.items():
            if name not in where_out or (name == "new" and in_place):
                continue
            aliases[len(ins)] = where_out[name]
            ins.append(("old_" + name, value, anywhere))
    names_in, names_out = tuple(x[0] for x in ins), tuple(x[0] for x in outs)
    cells = count * depth * width * levels
    results = pl.pallas_call(
        functools.partial(step_kernel, kind, names_in, names_out),
        grid=(count,),
        in_specs=[x[2] for x in ins],
        out_specs=[x[2] for x in outs],
        out_shape=[x[1] for x in outs],
        input_output_aliases=aliases,
        compiler_params=pltpu.CompilerParams(
            vmem_limit_bytes=VMEM_LIMIT, dimension_semantics=("arbitrary",)
        ),
        cost_estimate=pl.CostEstimate(flops=40 * cells, bytes_accessed=20 * cells, transcendentals=0),
        name="rows_" + kind,
    )(*[x[1] for x in ins])
    return dict(zip(names_out, results))


def sums_kernel(scale, u_ref, out_ref):
    for i in range(u_ref.shape[1]):
        total = u_ref[0, i]
        out_ref[0, i] = total * scale
        for j in range(1, u_ref.shape[0]):
            total = total + u_ref[j, i]
            out_ref[j, i] = total * scale


def add_kernel(scale, here_ref, below_ref, *refs):
    for i in range(here_ref.shape[1]):
        below = below_ref[0, i] * scale
        for j in range(here_ref.shape[0]):
            refs[-1][j, i] = here_ref[j, i] + below


def over_columns(body, u, extra, old, start, depth, name):
    n, _, width, levels = u.shape
    part = 2 if depth % 2 == 0 and start % 2 == 0 else 1
    block = pl.BlockSpec((n, part, width, levels), lambda i: (0, i + start // part, 0, 0))
    row = pl.BlockSpec((1, part, width, levels), lambda i: (0, i, 0, 0))
    operands = [u, *extra] + ([] if old is None else [old])
    specs = [block] + [row] * len(extra) + ([] if old is None else [pl.BlockSpec(memory_space=pl.ANY)])
    cells = n * depth * width * levels
    return pl.pallas_call(
        body,
        grid=(depth // part,),
        in_specs=specs,
        out_specs=block,
        out_shape=jax.ShapeDtypeStruct(u.shape, F32),
        input_output_aliases={} if old is None else {len(operands) - 1: 0},
        compiler_params=pltpu.CompilerParams(
            vmem_limit_bytes=VMEM_LIMIT, dimension_semantics=("arbitrary",)
        ),
        cost_estimate=pl.CostEstimate(flops=40 * cells, bytes_accessed=8 * cells, transcendentals=0),
        name=name,
    )(*operands)


def stage_kernel(*refs):
    half = len(refs) // 2
    for source, target in zip(refs[:half], refs[half:]):
        target[...] = source[...]


def staged(*arrays):
    shape = arrays[0].shape
    block = pl.BlockSpec((1,) + shape[1:], lambda j: (j, 0, 0, 0))
    size = arrays[0].size
    return pl.pallas_call(
        stage_kernel,
        grid=(shape[0],),
        in_specs=[block] * len(arrays),
        out_specs=[block] * len(arrays),
        out_shape=[jax.ShapeDtypeStruct(shape, F32)] * len(arrays),
        compiler_params=pltpu.CompilerParams(
            vmem_limit_bytes=STAGE_LIMIT, dimension_semantics=("arbitrary",)
        ),
        cost_estimate=pl.CostEstimate(flops=60 * size, bytes_accessed=24 * size, transcendentals=0),
        name="stage",
    )(*arrays)


def totals_below(total):
    peers = lax.axis_size("py")
    below = lax.ppermute(total, "py", [(i, i + 1) for i in range(peers - 1)])
    reach = 1
    while reach < peers - 1:
        below = below + lax.ppermute(below, "py", [(i, i + reach) for i in range(peers - reach)])
        reach *= 2
    return below


def exchange(faces):
    i_low, i_high, k_low, k_high = faces
    return (
        shift_up(i_high, "px"), shift_down(i_low, "px"),
        shift_up(k_high, "pz"), shift_down(k_low, "pz"),
    )


def local(field_now, earlier, speed_square):
    n, depth, width, _ = field_now.shape
    u, e, s = field_now, earlier, speed_square
    before = shift_up(u[n - 1 :], "py")
    after = shift_down(u[:1], "py")
    halos = exchange((u[:, :1], u[:, depth - 1 :], u[:, :, 0], u[:, :, width - 1]))
    u, e, s = staged(u, e, s)
    for step in range(STEPS):
        ending = step == STEPS - 1
        order = ("first", "middle", "last") if step % 2 == 0 else ("last", "middle", "first")
        state, total, rows = None, None, {}
        for kind in order:
            result = update(
                kind, u, e, s, halos, {"first": before, "last": after}.get(kind), state,
                step == 2, not ending, kind != "middle" and not (ending and kind == order[2]),
                total if ending else None,
            )
            if kind != "middle" and "row" in result:
                rows[kind] = result["row"]
            if ending:
                total = result.get("sum_out", result.get("row"))
                halves = result.get("sum_low"), result.get("sum_high")
            state = {name: result[name] for name in ("new",) + FACES if name in result}
        e, u = u, state["new"]
        if not ending:
            before = shift_up(rows["last"], "py")
            after = shift_down(rows["first"], "py")
            halos = exchange([state[name] for name in FACES])
    scale = 1.0 / (n * lax.axis_size("py"))
    low, high = [totals_below(half) for half in halves]
    here = over_columns(functools.partial(sums_kernel, scale), u, (), None, 0, depth, "sums_here")
    add = functools.partial(add_kernel, scale)
    out = over_columns(add, here, (low,), None, 0, depth // 2, "add_low")
    out = over_columns(add, here, (high,), out, depth // 2, depth - depth // 2, "add_high")
    return out, u


def solution(mesh):
    placed = P("py", "px", "pz", None)
    return jax.shard_map(
        local, mesh=mesh, in_specs=(placed, placed, placed), out_specs=(placed, placed), check_vma=False
    )
```

```python
import functools

import jax
import jax.numpy as jnp
from jax import lax
from jax.experimental import pallas as pl
from jax.experimental.pallas import tpu as pltpu
from jax.sharding import PartitionSpec as P

STEPS = 4
VMEM_LIMIT = 16 * 1024 * 1024
STAGE_LIMIT = 44 * 1024 * 1024
F32 = jnp.float32


def ring(axis, step):
    peers = lax.axis_size(axis)
    return [(i, (i + step) % peers) for i in range(peers)]


def shift_up(value, axis):
    return lax.ppermute(value, axis, ring(axis, 1))


def shift_down(value, axis):
    return lax.ppermute(value, axis, ring(axis, -1))


def update_row(at, below, above, before, speed, i_low, i_high, k_low, k_high, put, span):
    size, depth = i_low.shape[-2:], k_low.shape[0]
    place = lax.broadcasted_iota(jnp.int32, size, 0)
    first, last = place == 0, place == size[0] - 1
    for i in range(*span):
        middle = at(i)
        low = i_low[...] if i == 0 else at(i - 1)
        high = i_high[...] if i == depth - 1 else at(i + 1)
        back = jnp.where(first, k_low[i : i + 1, :], pltpu.roll(middle, 1, 0))
        ahead = jnp.where(last, k_high[i : i + 1, :], pltpu.roll(middle, size[0] - 1, 0))
        spread = below(i) + above(i) + low + high + back + ahead - 6.0 * middle
        put(i, 2.0 * middle - before(i) + speed(i) * spread)


def step_kernel(kind, span, names_in, names_out, *refs):
    r = dict(zip(names_in + names_out, refs))
    if kind == "middle":
        row = pl.program_id(0) + 1
        at = lambda i: r["u"][row, i]
        below = lambda i: r["u"][row - 1, i]
        above = lambda i: r["u"][row + 1, i]
    else:
        at = lambda i: r["u"][0, i]
        inner = lambda i: r["u_next"][0, i]
        outer = lambda i: r["halo"][0, i - span[0]]
        below, above = (outer, inner) if kind == "first" else (inner, outer)
    depth = r["k_low"].shape[1]
    width = r["i_low"].shape[2]

    if kind == "middle" and "sum_out" in r:

        @pl.when(pl.program_id(0) == 0)
        def _():
            r["sum_out"][...] = r["sum_in"][...]

    def put(i, new):
        if "new" in r:
            r["new"][0, i] = new
        if "row" in r:
            r["row"][0, i - span[0]] = new
        if "row_low" in r:
            cut = r["row_low"].shape[1]
            target = r["row_low"].at[0, i] if i < cut else r["row_high"].at[0, i - cut]
            target[...] = new
        if "sum_out" in r:
            r["sum_out"][0, i] = r["sum_out"][0, i] + new
        if "sum_part" in r:
            r["sum_part"][0, i - span[0]] = r["sum_in"][0, i] + new
        if "send_i_low" in r:
            if i == 0:
                r["send_i_low"][0, 0] = new
            if i == depth - 1:
                r["send_i_high"][0, 0] = new
            r["send_k_low"][0, i : i + 1, :] = new[:1]
            r["send_k_high"][0, i : i + 1, :] = new[width - 1 :]

    for i in range(span[0] if "given" in r else 0):
        r["new"][0, i] = r["given"][0, i]
    update_row(
        at, below, above, lambda i: r["e"][0, i], lambda i: r["s"][0, i],
        r["i_low"].at[0, 0], r["i_high"].at[0, 0], r["k_low"].at[0], r["k_high"].at[0], put, span,
    )


def part_of(depth):
    return max(1, 5 * depth // 8 // 2 * 2)


FACES = ("send_i_low", "send_i_high", "send_k_low", "send_k_high")


def update(kind, u, e, s, halos, halo, state, in_place, send, row_out, sum_in, span=None, given=None):
    n, depth, width, levels = u.shape
    start = {"first": 0, "middle": 1, "last": n - 1}[kind]
    count = n - 2 if kind == "middle" else 1
    line = pl.BlockSpec((1, depth, width, levels), lambda j: (j + start, 0, 0, 0))
    alone = pl.BlockSpec((1, depth, width, levels), lambda j: (0, 0, 0, 0))
    face_i = pl.BlockSpec((1, 1, width, levels), lambda j: (j + start, 0, 0, 0))
    face_k = pl.BlockSpec((1, depth, levels), lambda j: (j + start, 0, 0))
    anywhere = pl.BlockSpec(memory_space=pl.ANY)
    lone = lambda size: pl.BlockSpec((1, size, width, levels), lambda j: (0, 0, 0, 0))
    piece = lambda size: jax.ShapeDtypeStruct((1, size, width, levels), F32)
    early = span is not None and span[0] == 0
    low, high = span or (0, depth)
    ins = []
    if kind == "middle":
        ins.append(("u", u, pl.BlockSpec(u.shape, lambda j: (0, 0, 0, 0))))
    else:
        inner = start + 1 if kind == "first" else start - 1
        ins.append(("u", u, line))
        ins.append(("u_next", u, pl.BlockSpec((1, depth, width, levels), lambda j: (inner, 0, 0, 0))))
        ins.append(("halo", halo, lone(high - low)))
    source = state["new"] if (in_place and state) else e
    ins += [("e", source, line), ("s", s, line)]
    ins += [("i_low", halos[0], face_i), ("i_high", halos[1], face_i)]
    ins += [("k_low", halos[2], face_k), ("k_high", halos[3], face_k)]
    if sum_in is not None:
        ins.append(("sum_in", sum_in, alone))
    if given is not None:
        ins.append(("given", given, lone(low)))
    outs = [] if early else [("new", jax.ShapeDtypeStruct(u.shape, F32), line)]
    if send:
        face = jax.ShapeDtypeStruct((n, 1, width, levels), F32)
        strip = jax.ShapeDtypeStruct((n, depth, levels), F32)
        outs += list(zip(FACES, (face, face, strip, strip), (face_i, face_i, face_k, face_k)))
    if row_out == "parts":
        cut = part_of(depth)
        outs += [("row_low", piece(cut), lone(cut)), ("row_high", piece(depth - cut), lone(depth - cut))]
    elif row_out:
        outs.append(("row", piece(high - low), lone(high - low)))
    if sum_in is not None and kind == "middle":
        outs.append(("sum_out", jax.ShapeDtypeStruct((1, depth, width, levels), F32), alone))
    elif sum_in is not None:
        outs.append(("sum_part", piece(high - low), lone(high - low)))
    aliases = {}
    where_out = {name: index for index, (name, _, _) in enumerate(outs)}
    if in_place:
        aliases[[name for name, _, _ in ins].index("e")] = 0
    if state and not early:
        for name, value in state.items():
            if name not in where_out or (name == "new" and in_place):
                continue
            aliases[len(ins)] = where_out[name]
            ins.append(("old_" + name, value, anywhere))
    names_in, names_out = tuple(x[0] for x in ins), tuple(x[0] for x in outs)
    cells = count * depth * width * levels
    results = pl.pallas_call(
        functools.partial(step_kernel, kind, (low, high), names_in, names_out),
        grid=(count,),
        in_specs=[x[2] for x in ins],
        out_specs=[x[2] for x in outs],
        out_shape=[x[1] for x in outs],
        input_output_aliases=aliases,
        compiler_params=pltpu.CompilerParams(
            vmem_limit_bytes=VMEM_LIMIT, dimension_semantics=("arbitrary",)
        ),
        cost_estimate=pl.CostEstimate(flops=40 * cells, bytes_accessed=20 * cells, transcendentals=0),
        name="rows_" + kind,
    )(*[x[1] for x in ins])
    return dict(zip(names_out, results))


def sums_kernel(scale, u_ref, out_ref):
    for i in range(u_ref.shape[1]):
        total = u_ref[0, i]
        out_ref[0, i] = total * scale
        for j in range(1, u_ref.shape[0]):
            total = total + u_ref[j, i]
            out_ref[j, i] = total * scale


def add_kernel(scale, here_ref, below_ref, *refs):
    for i in range(here_ref.shape[1]):
        below = below_ref[0, i] * scale
        for j in range(here_ref.shape[0]):
            refs[-1][j, i] = here_ref[j, i] + below


def over_columns(body, u, extra, old, start, depth, name):
    n, _, width, levels = u.shape
    part = 2 if depth % 2 == 0 and start % 2 == 0 else 1
    block = pl.BlockSpec((n, part, width, levels), lambda i: (0, i + start // part, 0, 0))
    row = pl.BlockSpec((1, part, width, levels), lambda i: (0, i, 0, 0))
    operands = [u, *extra] + ([] if old is None else [old])
    specs = [block] + [row] * len(extra) + ([] if old is None else [pl.BlockSpec(memory_space=pl.ANY)])
    cells = n * depth * width * levels
    return pl.pallas_call(
        body,
        grid=(depth // part,),
        in_specs=specs,
        out_specs=block,
        out_shape=jax.ShapeDtypeStruct(u.shape, F32),
        input_output_aliases={} if old is None else {len(operands) - 1: 0},
        compiler_params=pltpu.CompilerParams(
            vmem_limit_bytes=VMEM_LIMIT, dimension_semantics=("arbitrary",)
        ),
        cost_estimate=pl.CostEstimate(flops=40 * cells, bytes_accessed=8 * cells, transcendentals=0),
        name=name,
    )(*operands)


def stage_kernel(*refs):
    half = len(refs) // 2
    for source, target in zip(refs[:half], refs[half:]):
        target[...] = source[...]


def staged(*arrays):
    shape = arrays[0].shape
    block = pl.BlockSpec((1,) + shape[1:], lambda j: (j, 0, 0, 0))
    size = arrays[0].size
    return pl.pallas_call(
        stage_kernel,
        grid=(shape[0],),
        in_specs=[block] * len(arrays),
        out_specs=[block] * len(arrays),
        out_shape=[jax.ShapeDtypeStruct(shape, F32)] * len(arrays),
        compiler_params=pltpu.CompilerParams(
            vmem_limit_bytes=STAGE_LIMIT, dimension_semantics=("arbitrary",)
        ),
        cost_estimate=pl.CostEstimate(flops=60 * size, bytes_accessed=24 * size, transcendentals=0),
        name="stage",
    )(*arrays)


def totals_below(total):
    peers = lax.axis_size("py")
    below = lax.ppermute(total, "py", [(i, i + 1) for i in range(peers - 1)])
    reach = 1
    while reach < peers - 1:
        below = below + lax.ppermute(below, "py", [(i, i + reach) for i in range(peers - reach)])
        reach *= 2
    return below


def exchange(faces):
    i_low, i_high, k_low, k_high = faces
    return (
        shift_up(i_high, "px"), shift_down(i_low, "px"),
        shift_up(k_high, "pz"), shift_down(k_low, "pz"),
    )


def local(field_now, earlier, speed_square):
    n, depth, width, _ = field_now.shape
    u, e, s = field_now, earlier, speed_square
    before = shift_up(u[n - 1 :], "py")
    after = shift_down(u[:1], "py")
    halos = exchange((u[:, :1], u[:, depth - 1 :], u[:, :, 0], u[:, :, width - 1]))
    u, e, s = staged(u, e, s)
    for step in range(STEPS):
        ending = step == STEPS - 1
        order = ("first", "middle", "last") if step % 2 == 0 else ("last", "middle", "first")
        state, total, rows = None, None, {}
        for kind in order:
            halo = {"first": before, "last": after}.get(kind)
            if ending and kind == order[2]:
                args = (kind, u, e, s, halos)
                cut = part_of(depth)
                start = update(*args, halo[0], state, False, False, True, total, (0, cut))
                rest = update(
                    *args, halo[1], state, False, False, False, total, (cut, depth), start["row"]
                )
                state = {"new": rest["new"]}
                parts = start["sum_part"], rest["sum_part"]
                continue
            row_out = kind != "middle"
            if step == STEPS - 2 and kind == order[2]:
                row_out = "parts"
            result = update(
                kind, u, e, s, halos, halo, state, step == 2, not ending, row_out,
                total if ending else None,
            )
            if row_out == "parts":
                rows[kind] = (result["row_low"], result["row_high"])
            elif row_out:
                rows[kind] = result["row"]
            if ending:
                total = result.get("sum_out", result.get("row"))
            state = {name: result[name] for name in ("new",) + FACES if name in result}
        e, u = u, state["new"]
        if not ending:
            before = jax.tree.map(lambda row: shift_up(row, "py"), rows["last"])
            after = jax.tree.map(lambda row: shift_down(row, "py"), rows["first"])
            halos = exchange([state[name] for name in FACES])
    scale = 1.0 / (n * lax.axis_size("py"))
    low, high = [totals_below(part) for part in parts]
    cut = part_of(depth)
    here = over_columns(functools.partial(sums_kernel, scale), u, (), None, 0, depth, "sums_here")
    add = functools.partial(add_kernel, scale)
    out = over_columns(add, here, (low,), None, 0, cut, "add_low")
    out = over_columns(add, here, (high,), out, cut, depth - cut, "add_high")
    return out, u


def solution(mesh):
    placed = P("py", "px", "pz", None)
    return jax.shard_map(
        local, mesh=mesh, in_specs=(placed, placed, placed), out_specs=(placed, placed), check_vma=False
    )
```

```python
import functools

import jax
import jax.numpy as jnp
from jax import lax
from jax.experimental import pallas as pl
from jax.experimental.pallas import tpu as pltpu
from jax.sharding import PartitionSpec as P

STEPS = 4
VMEM_LIMIT = 16 * 1024 * 1024
STAGE_LIMIT = 44 * 1024 * 1024
F32 = jnp.float32


def ring(axis, step):
    peers = lax.axis_size(axis)
    return [(i, (i + step) % peers) for i in range(peers)]


def shift_up(value, axis):
    return lax.ppermute(value, axis, ring(axis, 1))


def shift_down(value, axis):
    return lax.ppermute(value, axis, ring(axis, -1))


def update_row(at, below, above, before, speed, i_low, i_high, k_low, k_high, put, span):
    size, depth = i_low.shape[-2:], k_low.shape[0]
    place = lax.broadcasted_iota(jnp.int32, size, 0)
    first, last = place == 0, place == size[0] - 1
    for i in range(*span):
        middle = at(i)
        low = i_low[...] if i == 0 else at(i - 1)
        high = i_high[...] if i == depth - 1 else at(i + 1)
        back = jnp.where(first, k_low[i : i + 1, :], pltpu.roll(middle, 1, 0))
        ahead = jnp.where(last, k_high[i : i + 1, :], pltpu.roll(middle, size[0] - 1, 0))
        spread = below(i) + above(i) + low + high + back + ahead - 6.0 * middle
        put(i, 2.0 * middle - before(i) + speed(i) * spread)


def step_kernel(kind, span, names_in, names_out, *refs):
    r = dict(zip(names_in + names_out, refs))
    if kind == "middle":
        row = pl.program_id(0) + 1
        at = lambda i: r["u"][row, i]
        below = lambda i: r["u"][row - 1, i]
        above = lambda i: r["u"][row + 1, i]
    else:
        at = lambda i: r["u"][0, i]
        inner = lambda i: r["u_next"][0, i]
        outer = lambda i: r["halo"][0, i - span[0]]
        below, above = (outer, inner) if kind == "first" else (inner, outer)
    depth = r["k_low"].shape[1]
    width = r["i_low"].shape[2]

    if kind == "middle" and "sum_out" in r:

        @pl.when(pl.program_id(0) == 0)
        def _():
            r["sum_out"][...] = r["sum_in"][...]

    def put(i, new):
        if "new" in r:
            r["new"][0, i] = new
        if "row" in r:
            r["row"][0, i - span[0]] = new
        if "row_low" in r:
            cut = r["row_low"].shape[1]
            target = r["row_low"].at[0, i] if i < cut else r["row_high"].at[0, i - cut]
            target[...] = new
        if "sum_out" in r:
            r["sum_out"][0, i] = r["sum_out"][0, i] + new
        if "sum_part" in r:
            r["sum_part"][0, i - span[0]] = r["sum_in"][0, i] + new
        if "send_i_low" in r:
            if i == 0:
                r["send_i_low"][0, 0] = new
            if i == depth - 1:
                r["send_i_high"][0, 0] = new
            r["send_k_low"][0, i : i + 1, :] = new[:1]
            r["send_k_high"][0, i : i + 1, :] = new[width - 1 :]

    for i in range(span[0] if "given" in r else 0):
        r["new"][0, i] = r["given"][0, i]
    update_row(
        at, below, above, lambda i: r["e"][0, i], lambda i: r["s"][0, i],
        r["i_low"].at[0, 0], r["i_high"].at[0, 0], r["k_low"].at[0], r["k_high"].at[0], put, span,
    )


def part_of(depth):
    return max(1, 3 * depth // 4 // 2 * 2)


FACES = ("send_i_low", "send_i_high", "send_k_low", "send_k_high")


def update(kind, u, e, s, halos, halo, state, in_place, send, row_out, sum_in, span=None, given=None):
    n, depth, width, levels = u.shape
    start = {"first": 0, "middle": 1, "last": n - 1}[kind]
    count = n - 2 if kind == "middle" else 1
    line = pl.BlockSpec((1, depth, width, levels), lambda j: (j + start, 0, 0, 0))
    alone = pl.BlockSpec((1, depth, width, levels), lambda j: (0, 0, 0, 0))
    face_i = pl.BlockSpec((1, 1, width, levels), lambda j: (j + start, 0, 0, 0))
    face_k = pl.BlockSpec((1, depth, levels), lambda j: (j + start, 0, 0))
    anywhere = pl.BlockSpec(memory_space=pl.ANY)
    lone = lambda size: pl.BlockSpec((1, size, width, levels), lambda j: (0, 0, 0, 0))
    piece = lambda size: jax.ShapeDtypeStruct((1, size, width, levels), F32)
    early = span is not None and span[0] == 0
    low, high = span or (0, depth)
    ins = []
    if kind == "middle":
        ins.append(("u", u, pl.BlockSpec(u.shape, lambda j: (0, 0, 0, 0))))
    else:
        inner = start + 1 if kind == "first" else start - 1
        ins.append(("u", u, line))
        ins.append(("u_next", u, pl.BlockSpec((1, depth, width, levels), lambda j: (inner, 0, 0, 0))))
        ins.append(("halo", halo, lone(high - low)))
    source = state["new"] if (in_place and state) else e
    ins += [("e", source, line), ("s", s, line)]
    ins += [("i_low", halos[0], face_i), ("i_high", halos[1], face_i)]
    ins += [("k_low", halos[2], face_k), ("k_high", halos[3], face_k)]
    if sum_in is not None:
        ins.append(("sum_in", sum_in, alone))
    if given is not None:
        ins.append(("given", given, lone(low)))
    outs = [] if early else [("new", jax.ShapeDtypeStruct(u.shape, F32), line)]
    if send:
        face = jax.ShapeDtypeStruct((n, 1, width, levels), F32)
        strip = jax.ShapeDtypeStruct((n, depth, levels), F32)
        outs += list(zip(FACES, (face, face, strip, strip), (face_i, face_i, face_k, face_k)))
    if row_out == "parts":
        cut = part_of(depth)
        outs += [("row_low", piece(cut), lone(cut)), ("row_high", piece(depth - cut), lone(depth - cut))]
    elif row_out:
        outs.append(("row", piece(high - low), lone(high - low)))
    if sum_in is not None and kind == "middle":
        outs.append(("sum_out", jax.ShapeDtypeStruct((1, depth, width, levels), F32), alone))
    elif sum_in is not None:
        outs.append(("sum_part", piece(high - low), lone(high - low)))
    aliases = {}
    where_out = {name: index for index, (name, _, _) in enumerate(outs)}
    if in_place:
        aliases[[name for name, _, _ in ins].index("e")] = 0
    if state and not early:
        for name, value in state.items():
            if name not in where_out or (name == "new" and in_place):
                continue
            aliases[len(ins)] = where_out[name]
            ins.append(("old_" + name, value, anywhere))
    names_in, names_out = tuple(x[0] for x in ins), tuple(x[0] for x in outs)
    cells = count * depth * width * levels
    results = pl.pallas_call(
        functools.partial(step_kernel, kind, (low, high), names_in, names_out),
        grid=(count,),
        in_specs=[x[2] for x in ins],
        out_specs=[x[2] for x in outs],
        out_shape=[x[1] for x in outs],
        input_output_aliases=aliases,
        compiler_params=pltpu.CompilerParams(
            vmem_limit_bytes=VMEM_LIMIT, dimension_semantics=("arbitrary",)
        ),
        cost_estimate=pl.CostEstimate(flops=40 * cells, bytes_accessed=20 * cells, transcendentals=0),
        name="rows_" + kind,
    )(*[x[1] for x in ins])
    return dict(zip(names_out, results))


def sums_kernel(scale, u_ref, out_ref):
    for i in range(u_ref.shape[1]):
        total = u_ref[0, i]
        out_ref[0, i] = total * scale
        for j in range(1, u_ref.shape[0]):
            total = total + u_ref[j, i]
            out_ref[j, i] = total * scale


def add_kernel(scale, here_ref, below_ref, *refs):
    for i in range(here_ref.shape[1]):
        below = below_ref[0, i] * scale
        for j in range(here_ref.shape[0]):
            refs[-1][j, i] = here_ref[j, i] + below


def over_columns(body, u, extra, old, start, depth, name):
    n, _, width, levels = u.shape
    part = 2 if depth % 2 == 0 and start % 2 == 0 else 1
    block = pl.BlockSpec((n, part, width, levels), lambda i: (0, i + start // part, 0, 0))
    row = pl.BlockSpec((1, part, width, levels), lambda i: (0, i, 0, 0))
    operands = [u, *extra] + ([] if old is None else [old])
    specs = [block] + [row] * len(extra) + ([] if old is None else [pl.BlockSpec(memory_space=pl.ANY)])
    cells = n * depth * width * levels
    return pl.pallas_call(
        body,
        grid=(depth // part,),
        in_specs=specs,
        out_specs=block,
        out_shape=jax.ShapeDtypeStruct(u.shape, F32),
        input_output_aliases={} if old is None else {len(operands) - 1: 0},
        compiler_params=pltpu.CompilerParams(
            vmem_limit_bytes=VMEM_LIMIT, dimension_semantics=("arbitrary",)
        ),
        cost_estimate=pl.CostEstimate(flops=40 * cells, bytes_accessed=8 * cells, transcendentals=0),
        name=name,
    )(*operands)


def stage_kernel(*refs):
    half = len(refs) // 2
    for source, target in zip(refs[:half], refs[half:]):
        target[...] = source[...]


def staged(*arrays):
    shape = arrays[0].shape
    block = pl.BlockSpec((1,) + shape[1:], lambda j: (j, 0, 0, 0))
    size = arrays[0].size
    return pl.pallas_call(
        stage_kernel,
        grid=(shape[0],),
        in_specs=[block] * len(arrays),
        out_specs=[block] * len(arrays),
        out_shape=[jax.ShapeDtypeStruct(shape, F32)] * len(arrays),
        compiler_params=pltpu.CompilerParams(
            vmem_limit_bytes=STAGE_LIMIT, dimension_semantics=("arbitrary",)
        ),
        cost_estimate=pl.CostEstimate(flops=60 * size, bytes_accessed=24 * size, transcendentals=0),
        name="stage",
    )(*arrays)


def totals_below(total):
    peers = lax.axis_size("py")
    below = lax.ppermute(total, "py", [(i, i + 1) for i in range(peers - 1)])
    reach = 1
    while reach < peers - 1:
        below = below + lax.ppermute(below, "py", [(i, i + reach) for i in range(peers - reach)])
        reach *= 2
    return below


def exchange(faces):
    i_low, i_high, k_low, k_high = faces
    return (
        shift_up(i_high, "px"), shift_down(i_low, "px"),
        shift_up(k_high, "pz"), shift_down(k_low, "pz"),
    )


def local(field_now, earlier, speed_square):
    n, depth, width, _ = field_now.shape
    u, e, s = field_now, earlier, speed_square
    before = shift_up(u[n - 1 :], "py")
    after = shift_down(u[:1], "py")
    halos = exchange((u[:, :1], u[:, depth - 1 :], u[:, :, 0], u[:, :, width - 1]))
    u, e, s = staged(u, e, s)
    for step in range(STEPS):
        ending = step == STEPS - 1
        order = ("first", "middle", "last") if step % 2 == 0 else ("last", "middle", "first")
        state, total, rows = None, None, {}
        for kind in order:
            halo = {"first": before, "last": after}.get(kind)
            if ending and kind == order[2]:
                args = (kind, u, e, s, halos)
                cut = part_of(depth)
                start = update(*args, halo[0], state, False, False, True, total, (0, cut))
                rest = update(
                    *args, halo[1], state, False, False, False, total, (cut, depth), start["row"]
                )
                state = {"new": rest["new"]}
                parts = start["sum_part"], rest["sum_part"]
                continue
            row_out = kind != "middle"
            if step == STEPS - 2 and kind == order[2]:
                row_out = "parts"
            result = update(
                kind, u, e, s, halos, halo, state, step == 2, not ending, row_out,
                total if ending else None,
            )
            if row_out == "parts":
                rows[kind] = (result["row_low"], result["row_high"])
            elif row_out:
                rows[kind] = result["row"]
            if ending:
                total = result.get("sum_out", result.get("row"))
            state = {name: result[name] for name in ("new",) + FACES if name in result}
        e, u = u, state["new"]
        if not ending:
            before = jax.tree.map(lambda row: shift_up(row, "py"), rows["last"])
            after = jax.tree.map(lambda row: shift_down(row, "py"), rows["first"])
            halos = exchange([state[name] for name in FACES])
    scale = 1.0 / (n * lax.axis_size("py"))
    low, high = [totals_below(part) for part in parts]
    cut = part_of(depth)
    here = over_columns(functools.partial(sums_kernel, scale), u, (), None, 0, depth, "sums_here")
    add = functools.partial(add_kernel, scale)
    out = over_columns(add, here, (low,), None, 0, cut, "add_low")
    out = over_columns(add, here, (high,), out, cut, depth - cut, "add_high")
    return out, u


def solution(mesh):
    placed = P("py", "px", "pz", None)
    return jax.shard_map(
        local, mesh=mesh, in_specs=(placed, placed, placed), out_specs=(placed, placed), check_vma=False
    )
```
